256 devices in a mesh: batch: 32 (over y, x, core), rows: 8 (over z).
Axes of the slice: x: 4, y: 4, z: 8, core: 2. Of those that a mesh axis runs over, the one named last changes fastest.
Arguments:
- fine_level: bfloat16 [32, 64, 192, 384], P('batch', 'rows'), may hold values from -40 to 40
- middle_level: bfloat16 [32, 32, 96, 384], P('batch', 'rows'), may hold values from -40 to 40
- coarse_level: bfloat16 [32, 16, 48, 384], P('batch', 'rows'), may hold values from -40 to 40
- two_input_weights: float32 [2, 3, 2], replicated, may hold values from 0.5 to 2
- three_input_weights: float32 [2, 3], replicated, may hold values from 0.5 to 2
- depthwise: bfloat16 [2, 4, 3, 3, 384], replicated, may hold values from -2 to 2
- pointwise: bfloat16 [2, 4, 384, 384], replicated, may hold values from -0.3125 to 0.3125
- bn_gain: float32 [2, 4, 384], replicated, may hold values from 0.5 to 1.5
- bn_bias: float32 [2, 4, 384], replicated, may hold values from -3 to 3
Outputs:
- fine_result: bfloat16 [32, 64, 192, 384], P('batch', 'rows')
- middle_result: bfloat16 [32, 32, 96, 384], P('batch', 'rows')
- coarse_result: bfloat16 [32, 16, 48, 384], P('batch', 'rows')
The draws below stay inside these ranges and needn't reach their ends.
All inputs are finite; a program needn't handle non-finite values.
Results may differ from the reference program's by a relative error of at most 0.025.
Values may be sent and summed in bfloat16 or wider, within the bound.
No kernel may reach another device: no remote copies, remote signals or barrier semaphores. Data moves between devices by JAX's collectives and lax.ppermute only.
A program may use at most 64 MiB of HBM per device.

```python
import math
import jax
import jax.numpy as jnp
from jax import lax

C = 384
LAYERS = 2
COLS = 192
COLS_MID = 96
COLS_TOP = 48
HEIGHT = 64
HEIGHT_MID = 32
HEIGHT_TOP = 16
IMAGES = 32


def level_draw(key, height, width):
    noise_key = jax.random.fold_in(key, 11)
    channel_key = jax.random.fold_in(key, 12)
    offset_key = jax.random.fold_in(key, 13)
    shape = (IMAGES, height, width, C)
    noise = jnp.clip(jax.random.normal(noise_key, shape, jnp.float32), -4.0, 4.0)
    rise = math.log(3.0)
    channel_scale = jnp.exp(jax.random.uniform(channel_key, (C,), jnp.float32, math.log(0.3), math.log(3.0)))
    image_pos = jnp.arange(IMAGES, dtype=jnp.float32) / max(IMAGES - 1, 1)
    row_pos = jnp.arange(height, dtype=jnp.float32) / max(height - 1, 1)
    spatial_scale = jnp.exp(rise * (image_pos[:, None] + row_pos[None, :] - 1.0))
    offsets = 0.5 * jax.random.normal(offset_key, (IMAGES, 1, 1, C), jnp.float32)
    values = noise * spatial_scale[:, :, None, None] * channel_scale + offsets
    return jnp.clip(values, -40.0, 40.0).astype(jnp.bfloat16)


def draw_fine_level(key, part):
    return level_draw(key, HEIGHT, COLS)


def draw_middle_level(key, part):
    return level_draw(key, HEIGHT_MID, COLS_MID)


def draw_coarse_level(key, part):
    return level_draw(key, HEIGHT_TOP, COLS_TOP)


def gaussian(key, extent, scale, most, kind=jnp.bfloat16):
    entries = jax.random.normal(key, extent, jnp.float32) * scale
    return jnp.minimum(jnp.maximum(entries, -most), most).astype(kind)


def setup_inputs(seed: int = 0) -> dict:
    keys = jax.random.split(jax.random.key(seed), 10)
    return {
        "fine_level": draw_fine_level(jax.random.fold_in(keys[9], 71), 0),
        "middle_level": draw_middle_level(jax.random.fold_in(keys[9], 71), 0),
        "coarse_level": draw_coarse_level(jax.random.fold_in(keys[9], 71), 0),
        "two_input_weights": jnp.clip(jnp.exp(jax.random.uniform(keys[3], (LAYERS, 3, 2), jnp.float32, math.log(0.5), math.log(2.0))), 0.5, 2.0),
        "three_input_weights": jnp.clip(jnp.exp(jax.random.uniform(keys[4], (LAYERS, 3), jnp.float32, math.log(0.5), math.log(2.0))), 0.5, 2.0),
        "depthwise": gaussian(keys[5], (LAYERS, 4, 3, 3, C), 9 ** -0.5, 2.0),
        "pointwise": gaussian(keys[6], (LAYERS, 4, C, C), C ** -0.5, 0.3125),
        "bn_gain": jnp.clip(1.0 + 0.1 * jax.random.normal(keys[7], (LAYERS, 4, C), jnp.float32), 0.5, 1.5),
        "bn_bias": gaussian(keys[8], (LAYERS, 4, C), 0.5, 3.0, jnp.float32),
    }


def upsample(feature_maps):
    return jnp.repeat(jnp.repeat(feature_maps, 2, axis=1), 2, axis=2)

def reduce_resolution(feature_maps):
    lowest = jnp.array(-jnp.inf, feature_maps.dtype)
    padded = jnp.pad(feature_maps, ((0, 0), (0, 1), (0, 1), (0, 0)), constant_values=lowest)
    return lax.reduce_window(padded, lowest, lax.max, (1, 3, 3, 1), (1, 2, 2, 1), 'VALID')

def weighted_join_activate(inputs_list, weights):
    weight_sum = jnp.sum(weights) + 0.0001
    running = weights[0] * inputs_list[0].astype(jnp.float32)
    for position in range(1, len(inputs_list)):
        running = running + weights[position] * inputs_list[position].astype(jnp.float32)
    return jax.nn.silu(running / weight_sum).astype(jnp.bfloat16)

def separable(extended, kernel, projection):
    padded = jnp.pad(extended, ((0, 0), (0, 0), (1, 1), (0, 0)))
    height = extended.shape[1] - 2
    width = extended.shape[2]
    running = jnp.zeros((extended.shape[0], height, width, extended.shape[3]), jnp.float32)
    for row_tap in range(3):
        for col_tap in range(3):
            window = padded[:, row_tap:row_tap + height, col_tap:col_tap + width, :]
            running = running + window.astype(jnp.float32) * kernel[row_tap, col_tap].astype(jnp.float32)
    spatial = running.astype(jnp.bfloat16)
    projected = jnp.dot(spatial.reshape(-1, spatial.shape[-1]), projection, preferred_element_type=jnp.float32)
    return projected.reshape(spatial.shape)

def normalize(projected, gain, offset):
    center = lax.optimization_barrier(jnp.mean(projected, axis=(0, 1, 2)))
    centered = projected - center
    spread = lax.optimization_barrier(jnp.mean(centered * centered, axis=(0, 1, 2)))
    return (centered * lax.rsqrt(spread + 1e-05) * gain + offset).astype(jnp.bfloat16)

def node(activated, kernel, projection, gain, offset):
    padded = jnp.pad(activated, ((0, 0), (1, 1), (0, 0), (0, 0)))

    def one_image(image):
        return separable(image[None], kernel, projection)[0]
    projected = lax.map(one_image, padded)
    return normalize(projected, gain, offset)

def reference(fine_level, middle_level, coarse_level, two_input_weights, three_input_weights, depthwise, pointwise, bn_gain, bn_bias):
    fine, middle_grid, coarse_grid = (fine_level, middle_level, coarse_level)
    for bidirectional_layer in range(LAYERS):

        def run_layer_pair(index, activated):
            return node(activated, depthwise[bidirectional_layer, index], pointwise[bidirectional_layer, index], bn_gain[bidirectional_layer, index], bn_bias[bidirectional_layer, index])
        downward_middle = run_layer_pair(0, weighted_join_activate([middle_grid, upsample(coarse_grid)], two_input_weights[bidirectional_layer, 0]))
        updated_fine = run_layer_pair(1, weighted_join_activate([fine, upsample(downward_middle)], two_input_weights[bidirectional_layer, 1]))
        updated_middle = run_layer_pair(2, weighted_join_activate([middle_grid, downward_middle, reduce_resolution(updated_fine)], three_input_weights[bidirectional_layer]))
        updated_coarse = run_layer_pair(3, weighted_join_activate([coarse_grid, reduce_resolution(updated_middle)], two_input_weights[bidirectional_layer, 2]))
        fine, middle_grid, coarse_grid = (updated_fine, updated_middle, updated_coarse)
    return (fine, middle_grid, coarse_grid)
```

```python
import functools

import jax
import jax.numpy as jnp
from jax import lax
from jax.experimental import pallas as pl
from jax.experimental.pallas import tpu as pltpu
from jax.sharding import Mesh
from jax.sharding import PartitionSpec as P

LAYERS = 2
C = 384
T = 48
BATCH = ("batch_0", "batch_1", "batch_2")
FIRST = ("batch_0", "batch_1")
SECOND = ("batch_2", "rows")
F32 = jnp.float32
BF16 = jnp.bfloat16
LOW = -3.0e38


def vspec():
    return pl.BlockSpec(memory_space=pltpu.VMEM)


def sspec():
    return pl.BlockSpec(memory_space=pltpu.SMEM)


def from_left(plane):
    rolled = pltpu.roll(plane, 1, 0)
    at = lax.broadcasted_iota(jnp.int32, plane.shape, 0)
    return jnp.where(at == 0, 0.0, rolled)


def from_right(plane, fill=0.0):
    rolled = pltpu.roll(plane, plane.shape[0] - 1, 0)
    at = lax.broadcasted_iota(jnp.int32, plane.shape, 0)
    return jnp.where(at == plane.shape[0] - 1, fill, rolled)


def affine_of(totals_ref, gain, bias, count):
    totals = jnp.sum(totals_ref[...], axis=0)
    center = totals[:, :C] * (1.0 / count)
    spread = totals[:, C:] * (1.0 / count) - center * center
    scale = lax.rsqrt(spread + 1e-05) * gain
    return scale, bias - center * scale


def activate(half):
    return half + half * jnp.tanh(half)


def up32(x):
    return x.astype(F32)


def gain_bias(gain_ref, bias_ref, layer, n):
    return gain_ref[layer, n : n + 1, :], bias_ref[layer, n : n + 1, :]


def put_stats(stats_ref, total, square):
    line = jnp.concatenate([total, square], axis=1)
    for k in range(16):
        stats_ref[k] = line


def column_sum(x):
    return jnp.sum(x, axis=0, keepdims=True)


def conv_row(act_ref, taps, h, phases):
    out = []
    for f in range(phases):
        acc = None
        for j in (0, 2, 1):
            src, shift = f + j - 1, None
            if src < 0:
                src, shift = phases - 1, from_left
            elif src >= phases:
                src, shift = 0, from_right
            part = None
            for i in range(3):
                term = act_ref[h + i, src] * taps[i * 3 + j]
                part = term if part is None else part + term
            if shift is not None:
                part = shift(part)
            acc = part if acc is None else acc + part
        out.append(acc)
    return out


def load_taps(dw_ref, layer, n):
    return [up32(dw_ref[layer, n, i, j : j + 1, :]) for i in range(3) for j in range(3)]


def deinterleave(row, perm):
    return jnp.dot(perm, row, preferred_element_type=F32).astype(BF16)


def one_hot(width, phases, inverse=False):
    r = lax.broadcasted_iota(jnp.int32, (width, width), 0)
    c = lax.broadcasted_iota(jnp.int32, (width, width), 1)
    if inverse:
        r, c = c, r
    want = lax.rem(r, T) * phases + lax.div(r, T)
    return jnp.where(want == c, 1.0, 0.0).astype(BF16)


def prep_fine_kernel(x_ref, o_ref):
    perm = one_hot(4 * T, 4)

    def row(h, _):
        o_ref[h] = deinterleave(x_ref[0, h], perm).reshape(4, T, C)
        return 0

    lax.fori_loop(0, 8, row, 0)


def prep_mid_kernel(x_ref, up_ref, down_ref, o_ref):
    perm = one_hot(2 * T, 2)
    o_ref[0] = deinterleave(up_ref[: 2 * T, :], perm).reshape(2, T, C)
    for h in range(4):
        o_ref[h + 1] = deinterleave(x_ref[0, h], perm).reshape(2, T, C)
    o_ref[5] = deinterleave(down_ref[: 2 * T, :], perm).reshape(2, T, C)


def out_kernel(phases, rows, x_ref, aff_ref, o_ref):
    perm = one_hot(phases * T, phases, inverse=True)
    scale, shift = aff_ref[0:1, :], aff_ref[1:2, :]

    def row(h, _):
        planes = (up32(x_ref[h].reshape(phases * T, C)) * scale + shift).astype(BF16)
        o_ref[0, h] = jnp.dot(perm, planes, preferred_element_type=F32).astype(BF16)
        return 0

    lax.fori_loop(0, rows, row, 0)


def out_top_kernel(layer, count, x_ref, totals_ref, gain_ref, bias_ref, o_ref):
    scale, shift = affine_of(totals_ref, *gain_bias(gain_ref, bias_ref, layer, 3), count)
    for h in range(2):
        o_ref[0, h] = (up32(x_ref[h]) * scale + shift).astype(BF16)


def finish_small(act_ref, spatial_ref, p_ref, stats_ref, dw_ref, pw_ref, layer, n, rows, phases):
    taps = load_taps(dw_ref, layer, n)
    for h in range(rows):
        for f, plane in enumerate(conv_row(act_ref, taps, h, phases)):
            at = (h * phases + f) * T
            spatial_ref[at : at + T, :] = plane.astype(BF16)
    projected = jnp.dot(spatial_ref[...], pw_ref[layer, n], preferred_element_type=F32)
    put_stats(stats_ref, column_sum(projected), column_sum(projected * projected))
    p_ref[...] = projected.astype(BF16).reshape(p_ref.shape)


def k0_kernel(
    layer,
    count,
    flags_ref,
    w_ref,
    mid_above_ref,
    mid_ref,
    mid_below_ref,
    top_above_ref,
    top_ref,
    top_below_ref,
    mid_aff_ref,
    totals_ref,
    gain_ref,
    bias_ref,
    dw_ref,
    pw_ref,
    p_ref,
    stats_ref,
    aff_ref,
    act_ref,
    spatial_ref,
):
    w0, w1 = w_ref[layer * 6], w_ref[layer * 6 + 1]
    norm = 0.5 / (w0 + w1 + 0.0001)
    w0, w1 = w0 * norm, w1 * norm
    if layer:
        scale, shift = affine_of(totals_ref, *gain_bias(gain_ref, bias_ref, layer - 1, 3), count)
        aff_ref[0:1, :] = scale
        aff_ref[1:2, :] = shift
        a = mid_aff_ref[0:1, :] * w0
        b = scale * w1
        c = mid_aff_ref[1:2, :] * w0 + shift * w1
    else:
        aff_ref[...] = jnp.zeros(aff_ref.shape, F32)
        a, b, c = w0, w1, 0.0
    up_flag, down_flag = flags_ref[0], flags_ref[1]

    def top_row(i):
        if i < 0:
            return up32(top_above_ref[...])
        return up32(top_below_ref[...]) if i > 1 else up32(top_ref[i])

    for i in range(-1, 3):
        u = top_row(i) * b + c
        for r in (2 * i, 2 * i + 1):
            if r < -1 or r > 4:
                continue
            for p in range(2):
                if r < 0:
                    m = mid_above_ref[p]
                elif r > 3:
                    m = mid_below_ref[p]
                else:
                    m = mid_ref[r, p]
                act = activate(up32(m) * a + u)
                if r < 0:
                    act = act * up_flag
                elif r > 3:
                    act = act * down_flag
                act_ref[r + 1, p] = act
    finish_small(act_ref, spatial_ref, p_ref, stats_ref, dw_ref, pw_ref, layer, 0, 4, 2)


def k1_kernel(
    layer,
    count,
    flags_ref,
    w_ref,
    fine_above_ref,
    fine_ref,
    fine_below_ref,
    td_above_ref,
    td_ref,
    td_below_ref,
    fine_aff_ref,
    totals_ref,
    gain_ref,
    bias_ref,
    dw_ref,
    pw_ref,
    p_ref,
    stats_ref,
    aff_ref,
    u_ref,
    act_ref,
    spatial_ref,
):
    w0, w1 = w_ref[layer * 6 + 2], w_ref[layer * 6 + 3]
    norm = 0.5 / (w0 + w1 + 0.0001)
    w0, w1 = w0 * norm, w1 * norm
    scale, shift = affine_of(totals_ref, *gain_bias(gain_ref, bias_ref, layer, 0), count)
    aff_ref[0:1, :] = scale
    aff_ref[1:2, :] = shift
    b, c = scale * w1, shift * w1
    if layer:
        a = fine_aff_ref[0:1, :] * w0
        c = c + fine_aff_ref[1:2, :] * w0
    else:
        a = w0
    for p in range(2):
        u_ref[0, p] = up32(td_above_ref[p]) * b + c
        for i in range(4):
            u_ref[i + 1, p] = up32(td_ref[i, p]) * b + c
        u_ref[5, p] = up32(td_below_ref[p]) * b + c
    up_flag, down_flag = flags_ref[0], flags_ref[1]
    for f in range(4):
        act_ref[0, f] = activate(up32(fine_above_ref[f]) * a + u_ref[0, f // 2]) * up_flag
        act_ref[9, f] = activate(up32(fine_below_ref[f]) * a + u_ref[5, f // 2]) * down_flag

    def act_row(i, _):
        for q in range(2):
            for f in range(4):
                h = 2 * i + q
                act_ref[h + 1, f] = activate(up32(fine_ref[h, f]) * a + u_ref[i + 1, f // 2])
        return 0

    lax.fori_loop(0, 4, act_row, 0)
    taps = load_taps(dw_ref, layer, 1)

    def conv(h, carry):
        total, square = carry
        for f, plane in enumerate(conv_row(act_ref, taps, h, 4)):
            spatial_ref[f * T : (f + 1) * T, :] = plane.astype(BF16)
        projected = jnp.dot(spatial_ref[...], pw_ref[layer, 1], preferred_element_type=F32)
        p_ref[h] = projected.astype(BF16).reshape(4, T, C)
        return total + column_sum(projected), square + column_sum(projected * projected)

    zero = jnp.zeros((1, C), F32)
    total, square = lax.fori_loop(0, 8, conv, (zero, zero))
    put_stats(stats_ref, total, square)


def pool_fine_kernel(p_ref, up_ref, pool_ref):
    def column_pool(h):
        x = [up32(p_ref[h, f]) for f in range(4)]
        even = jnp.maximum(jnp.maximum(x[0], x[1]), x[2])
        odd = jnp.maximum(jnp.maximum(x[2], x[3]), from_right(x[0], LOW))
        return even, odd

    first = column_pool(0)
    upper = first
    for i in range(4):
        rows = [upper, column_pool(2 * i + 1)]
        if i < 3:
            upper = column_pool(2 * i + 2)
            rows.append(upper)
        for p in range(2):
            best = functools.reduce(jnp.maximum, [r[p] for r in rows]).astype(BF16)
            pool_ref[i, p] = best
            if i == 0:
                up_ref[0, p] = first[p].astype(BF16)
                up_ref[1, p] = best


def pool_mid_kernel(p_ref, up_ref, pool_ref):
    def column_pool(h):
        x = [up32(p_ref[h, f]) for f in range(2)]
        return jnp.maximum(jnp.maximum(x[0], x[1]), from_right(x[0], LOW))

    rows = [column_pool(h) for h in range(4)]
    best = jnp.maximum(jnp.maximum(rows[0], rows[1]), rows[2]).astype(BF16)
    pool_ref[0] = best
    pool_ref[1] = jnp.maximum(rows[2], rows[3]).astype(BF16)
    up_ref[0] = rows[0].astype(BF16)
    up_ref[1] = best


def k2_kernel(
    layer,
    count,
    flags_ref,
    w_ref,
    mid_above_ref,
    mid_ref,
    mid_below_ref,
    td_above_ref,
    td_ref,
    td_below_ref,
    pool_above_ref,
    pool_ref,
    pool_own_ref,
    pool_below_ref,
    mid_aff_ref,
    td_aff_ref,
    totals_ref,
    gain_ref,
    bias_ref,
    dw_ref,
    pw_ref,
    p_ref,
    stats_ref,
    aff_ref,
    act_ref,
    spatial_ref,
):
    w0, w1, w2 = (w_ref[12 + layer * 3 + k] for k in range(3))
    norm = 0.5 / (w0 + w1 + w2 + 0.0001)
    w0, w1, w2 = w0 * norm, w1 * norm, w2 * norm
    scale, shift = affine_of(totals_ref, *gain_bias(gain_ref, bias_ref, layer, 1), count)
    aff_ref[0:1, :] = scale
    aff_ref[1:2, :] = shift
    b = td_aff_ref[0:1, :] * w1
    d = scale * w2
    c = td_aff_ref[1:2, :] * w1 + shift * w2
    if layer:
        a = mid_aff_ref[0:1, :] * w0
        c = c + mid_aff_ref[1:2, :] * w0
    else:
        a = w0
    up_flag, down_flag = flags_ref[0], flags_ref[1]
    for r in range(-1, 5):
        for p in range(2):
            if r < 0:
                m, td = mid_above_ref[p], td_above_ref[p]
                pool = jnp.maximum(up32(pool_above_ref[p]), up32(pool_own_ref[0, p]))
            elif r > 3:
                m, td = mid_below_ref[p], td_below_ref[p]
                pool = up32(pool_below_ref[1, p])
            else:
                m, td = mid_ref[r, p], td_ref[r, p]
                pool = up32(pool_ref[r, p])
                if r == 3:
                    below = jnp.where(down_flag > 0.5, up32(pool_below_ref[0, p]), LOW)
                    pool = jnp.maximum(pool, below)
            act = activate(up32(m) * a + up32(td) * b + (pool * d + c))
            if r < 0:
                act = act * up_flag
            elif r > 3:
                act = act * down_flag
            act_ref[r + 1, p] = act
    finish_small(act_ref, spatial_ref, p_ref, stats_ref, dw_ref, pw_ref, layer, 2, 4, 2)


def k3_kernel(
    layer,
    count,
    flags_ref,
    w_ref,
    top_above_ref,
    top_ref,
    top_below_ref,
    pool_above_ref,
    pool_ref,
    pool_own_ref,
    pool_below_ref,
    top_aff_ref,
    totals_ref,
    gain_ref,
    bias_ref,
    dw_ref,
    pw_ref,
    p_ref,
    stats_ref,
    aff_ref,
    act_ref,
    spatial_ref,
):
    w0, w1 = w_ref[layer * 6 + 4], w_ref[layer * 6 + 5]
    norm = 0.5 / (w0 + w1 + 0.0001)
    w0, w1 = w0 * norm, w1 * norm
    scale, shift = affine_of(totals_ref, *gain_bias(gain_ref, bias_ref, layer, 2), count)
    aff_ref[0:1, :] = scale
    aff_ref[1:2, :] = shift
    d, c = scale * w1, shift * w1
    if layer:
        a = top_aff_ref[0:1, :] * w0
        c = c + top_aff_ref[1:2, :] * w0
    else:
        a = w0
    up_flag, down_flag = flags_ref[0], flags_ref[1]
    for r in range(-1, 3):
        if r < 0:
            m = top_above_ref[...]
            pool = jnp.maximum(up32(pool_above_ref[...]), up32(pool_own_ref[0]))
        elif r > 1:
            m = top_below_ref[...]
            pool = up32(pool_below_ref[1])
        else:
            m = top_ref[r]
            pool = up32(pool_ref[r])
            if r == 1:
                below = jnp.where(down_flag > 0.5, up32(pool_below_ref[0]), LOW)
                pool = jnp.maximum(pool, below)
        act = activate(up32(m) * a + (pool * d + c))
        if r < 0:
            act = act * up_flag
        elif r > 1:
            act = act * down_flag
        act_ref[r + 1, 0] = act
    finish_small(act_ref, spatial_ref, p_ref, stats_ref, dw_ref, pw_ref, layer, 3, 2, 1)


def call(kernel, outs, args, scalars=0, scratch=(), flops=1_000_000, name=None):
    single = isinstance(outs, tuple)
    shapes = [outs] if single else list(outs)
    result = pl.pallas_call(
        kernel,
        out_shape=[jax.ShapeDtypeStruct(s, d) for s, d in shapes],
        in_specs=[sspec()] * scalars + [vspec()] * (len(args) - scalars),
        out_specs=[vspec()] * len(shapes),
        scratch_shapes=list(scratch),
        compiler_params=pltpu.CompilerParams(vmem_limit_bytes=24 * 1024 * 1024),
        cost_estimate=pl.CostEstimate(flops=flops, bytes_accessed=1_000_000, transcendentals=0),
        name=name,
    )(*args)
    return result[0] if single else result


STATS = ((16, 1, 2 * C), F32)
AFF = ((2, C), F32)


def exchange(stats, axis):
    return lax.all_to_all(stats, axis, split_axis=0, concat_axis=0, tiled=True)


def reduce_stats(stats):
    near = exchange(stats, FIRST).sum(axis=0, keepdims=True)
    return exchange(jnp.broadcast_to(near, stats.shape), SECOND)


def send_down(x):
    n = lax.axis_size("rows")
    return lax.ppermute(x, "rows", [(i, i + 1) for i in range(n - 1)])


def send_up(x):
    n = lax.axis_size("rows")
    return lax.ppermute(x, "rows", [(i + 1, i) for i in range(n - 1)])


def small_scratch(rows, phases):
    return (
        pltpu.VMEM((rows + 2, phases, T, C), F32),
        pltpu.VMEM((rows * phases * T, C), BF16),
    )


def body(fine_in, mid_in, top_in, two, three, dw, pw, gain, bias):
    devices = lax.axis_size(BATCH) * lax.axis_size("rows")
    fine_count, mid_count, top_count = (float(k * T * devices) for k in (32, 8, 2))
    row = lax.axis_index("rows")
    flags = jnp.stack([row > 0, row < lax.axis_size("rows") - 1]).astype(F32)
    weights = jnp.concatenate([two.reshape(-1), three.reshape(-1)])
    no_aff = jnp.zeros((2, C), F32)
    no_totals = jnp.zeros((16, 1, 2 * C), F32)

    from_above = send_down(jnp.concatenate([mid_in[0, 3], top_in[0, 1]], axis=0))
    from_below = send_up(jnp.concatenate([mid_in[0, 0], top_in[0, 0]], axis=0))
    fine = call(prep_fine_kernel, ((8, 4, T, C), BF16), [fine_in], flops=6_000_000, name="prep_fine")
    mid_all = call(
        prep_mid_kernel, ((6, 2, T, C), BF16), [mid_in, from_above, from_below], name="prep_mid"
    )
    mid = (mid_all[0], mid_all[1:5], mid_all[5])
    top = (from_above[2 * T :], top_in[0], from_below[2 * T :])
    mid_aff, top_aff, fine_aff = no_aff, no_aff, no_aff
    top_totals = no_totals
    params = [gain, bias, dw, pw]
    fine_halo = None

    for layer in range(LAYERS):
        last = layer == LAYERS - 1
        p0, stats, new_top_aff = call(
            functools.partial(k0_kernel, layer, top_count),
            [((4, 2, T, C), BF16), STATS, AFF],
            [flags, weights, *mid, *top, mid_aff, top_totals, *params],
            scalars=2,
            scratch=small_scratch(4, 2),
            name=f"node0_{layer}",
        )
        top_aff = new_top_aff
        td = (send_down(p0[3]), p0, send_up(p0[0]))
        if fine_halo is None:
            fine_halo = (send_down(fine[7]), send_up(fine[0]))
        totals = reduce_stats(stats)

        p1, stats, td_aff = call(
            functools.partial(k1_kernel, layer, mid_count),
            [((8, 4, T, C), BF16), STATS, AFF],
            [flags, weights, fine_halo[0], fine, fine_halo[1], *td, fine_aff, totals, *params],
            scalars=2,
            scratch=(
                pltpu.VMEM((6, 2, T, C), F32),
                pltpu.VMEM((10, 4, T, C), F32),
                pltpu.VMEM((4 * T, C), BF16),
            ),
            flops=4_000_000,
            name=f"node1_{layer}",
        )
        pool_up, pool = call(
            pool_fine_kernel,
            [((2, 2, T, C), BF16), ((4, 2, T, C), BF16)],
            [p1],
            flops=2_000_000,
            name=f"pool_fine_{layer}",
        )
        pool_args = (send_down(pool[3]), pool, pool_up, send_up(pool_up))
        totals = reduce_stats(stats)

        p2, stats, fine_aff = call(
            functools.partial(k2_kernel, layer, fine_count),
            [((4, 2, T, C), BF16), STATS, AFF],
            [flags, weights, *mid, *td, *pool_args, mid_aff, td_aff, totals, *params],
            scalars=2,
            scratch=small_scratch(4, 2),
            name=f"node2_{layer}",
        )
        pool_up, pool = call(
            pool_mid_kernel,
            [((2, T, C), BF16), ((2, T, C), BF16)],
            [p2],
            name=f"pool_mid_{layer}",
        )
        pool_args = (send_down(pool[1]), pool, pool_up, send_up(pool_up))
        if last:
            fine_out = call(
                functools.partial(out_kernel, 4, 8),
                ((1, 8, 4 * T, C), BF16),
                [p1, fine_aff],
                flops=6_000_000,
                name="out_fine",
            )
        else:
            mid_next = (send_down(p2[3]), p2, send_up(p2[0]))
        totals = reduce_stats(stats)

        p3, stats, mid_aff = call(
            functools.partial(k3_kernel, layer, mid_count),
            [((2, T, C), BF16), STATS, AFF],
            [flags, weights, *top, *pool_args, top_aff, totals, *params],
            scalars=2,
            scratch=small_scratch(2, 1),
            name=f"node3_{layer}",
        )
        if last:
            mid_out = call(
                functools.partial(out_kernel, 2, 4),
                ((1, 4, 2 * T, C), BF16),
                [p2, mid_aff],
                flops=2_000_000,
                name="out_mid",
            )
        else:
            top = (send_down(p3[1]), p3, send_up(p3[0]))
            mid = mid_next
            fine = p1
            fine_halo = (send_down(p1[7]), send_up(p1[0]))
        top_totals = reduce_stats(stats)

    top_out = call(
        functools.partial(out_top_kernel, LAYERS - 1, top_count),
        ((1, 2, T, C), BF16),
        [p3, top_totals, gain, bias],
        name="out_top",
    )
    return fine_out, mid_out, top_out


def solution(mesh):
    split = Mesh(
        mesh.devices.reshape(4, 4, 2, mesh.shape["rows"]), ("batch_0", "batch_1", "batch_2", "rows")
    )
    level = P(BATCH, "rows", None, None)
    in_specs = (level,) * 3 + (P(),) * 6
    return jax.shard_map(
        body, mesh=split, in_specs=in_specs, out_specs=(level,) * 3, check_vma=False
    )
```
